32 devices in a mesh: row: 8 (over y, x, core), depth: 4 (over z).
Axes of the slice: x: 2, y: 2, z: 4, core: 2. Of those that a mesh axis runs over, the one named last changes fastest.
Arguments:
- l_cores: float32 [16, 32, 384, 384], P('row', 'depth'), may hold values from -0.0546875 to 0.0546875
- l_bucket: int32 [16, 32], P('row', 'depth'), may hold values from 1 to 3
- present: int32 [16, 32], P('row', 'depth'), may hold values 0 or 1
- u_cores: float32 [32, 4, 384, 384], P('depth', None, 'row'), may hold values from -6 to 6
- u_bucket: int32 [32, 4], P('depth'), may hold values from 1 to 3
- diag_cores: float32 [16, 4, 384, 384], P('row', None, 'depth'), may hold values from -6 to 6
- pivot_inv: float32 [4, 384, 384], P(None, 'row'), may hold values from -0.3125 to 0.3125
- coupling: float32 [3, 384, 384], P(None, 'row'), may hold values from -0.21875 to 0.21875
Outputs:
- finished: float32 [16, 4, 384, 384], P('row', None, 'depth')
The draws below stay inside these ranges and needn't reach their ends.
Inputs may be any that keep to these rules, and one draw needn't show every extreme that they name: A lower tile's core rank is l_bucket * 128. An upper tile's core rank is u_bucket * 128. `present`: 1 marks a nonzero lower tile.
All inputs are finite; a program needn't handle non-finite values. No bound on the sum of `present` on one device may be relied on, other than what follows from the above.
Results may differ from the reference program's by a relative error of at most 0.0003.
Values sent between devices are 32-bit elements; how exact they have to be, the bound alone decides.
No kernel may reach another device: no remote copies, remote signals or barrier semaphores. Data moves between devices by JAX's collectives and lax.ppermute only.
A program may use at most 128 MiB of HBM per device.

```python
import jax
import jax.numpy as jnp
from jax import lax

R = 384
COLS = 4
TROWS = 16
PIVOTS = 32


def place_ends(entries, stream_key, least, top_value):
    extent = entries.shape
    index_at = [jax.random.randint(jax.random.fold_in(stream_key, axis), (), 0, extent[axis]) for axis in range(len(extent))]
    entries = entries.at[tuple(index_at)].set(least)
    longest = extent.index(max(extent))
    index_at[longest] = (index_at[longest] + 1) % extent[longest]
    return entries.at[tuple(index_at)].set(top_value)


def shard_levels(key, extent, pieces, low, high):
    gain = 1.0
    for dim, blocks in pieces:
        steps = jax.random.uniform(jax.random.fold_in(jax.random.fold_in(key, 6), dim), (blocks,), jnp.float32, low / len(pieces), high / len(pieces))
        gain = gain * jnp.repeat(jnp.exp(steps), extent[dim] // blocks).reshape((-1,) + (1,) * (len(extent) - 1 - dim))
    return gain


def noise(key, extent, scale, limit, shards=(), kind=jnp.bfloat16):
    array = scale * jax.random.normal(key, extent, jnp.float32)
    if shards:
        array = array * shard_levels(key, extent, shards, -0.22, 0.18)
    return jnp.clip(array, -limit, limit).astype(kind)


def setup_inputs(seed: int = 0) -> dict:
    key_of = jax.random.split(jax.random.key(seed), 9)
    return {
        "l_cores": noise(key_of[0], (TROWS, PIVOTS, R, R), (R * PIVOTS) ** -0.5, 0.0546875, ((0, 8), (1, 4)), jnp.float32),
        "l_bucket": place_ends(jax.random.randint(key_of[1], (TROWS, PIVOTS), 1, 4), jax.random.fold_in(key_of[1], 1), 1, 3).astype(jnp.int32),
        "present": place_ends((jax.random.randint(key_of[2], (TROWS, PIVOTS), 0, 4) < 3).astype(jnp.int32), jax.random.fold_in(key_of[2], 1), 0, 1),
        "u_cores": noise(key_of[3], (PIVOTS, COLS, R, R), 1.0, 6.0, ((0, 4), (2, 8)), jnp.float32),
        "u_bucket": place_ends(jax.random.randint(key_of[4], (PIVOTS, COLS), 1, 4), jax.random.fold_in(key_of[4], 1), 1, 3).astype(jnp.int32),
        "diag_cores": noise(key_of[5], (TROWS, COLS, R, R), 1.0, 6.0, ((0, 8), (2, 4)), jnp.float32),
        "pivot_inv": noise(key_of[6], (COLS, R, R), R ** -0.5, 0.3125, ((1, 8),), jnp.float32),
        "coupling": noise(key_of[7], (COLS - 1, R, R), (2 * R) ** -0.5, 0.21875, ((1, 8),), jnp.float32),
    }


HIGH = lax.Precision.HIGHEST


def reference(l_cores, l_bucket, present, u_cores, u_bucket, diag_cores, pivot_inv, coupling):
    rank_step = R // 3
    positions = jnp.arange(R, dtype=jnp.int32)
    u_keep = (positions[None, None, :] < (u_bucket * rank_step)[:, :, None]).astype(jnp.float32)
    u_masked = u_cores * u_keep[..., None]

    def one_row(inputs):
        cores, buckets, flags, targets = inputs
        col_keep = ((positions[None, :] < (buckets * rank_step)[:, None]) & (flags[:, None] > 0)).astype(jnp.float32)
        masked = cores * col_keep[:, None, :]
        updates = jnp.einsum("kar,kjrb->jab", masked, u_masked, precision=HIGH)
        reduced = targets - updates
        previous = jnp.dot(reduced[0], pivot_inv[0], precision=HIGH, preferred_element_type=jnp.float32)
        results = [previous]
        for column in range(1, COLS):
            linked = jnp.dot(previous, coupling[column - 1], precision=HIGH, preferred_element_type=jnp.float32)
            previous = jnp.dot(reduced[column] - linked, pivot_inv[column], precision=HIGH, preferred_element_type=jnp.float32)
            results.append(previous)
        return jnp.stack(results)

    return lax.map(one_row, (l_cores, l_bucket, present, diag_cores))
```

```python
import functools

import jax
import jax.numpy as jnp
from jax import lax
from jax.experimental import pallas as pl
from jax.experimental.pallas import tpu as pltpu
from jax.sharding import PartitionSpec as P


HIGH = lax.Precision.HIGHEST
F32 = jnp.float32
BF16 = jnp.bfloat16


def plain_device(l_cores, l_bucket, present, u_cores, u_bucket, diag_cores, pivot_inv, coupling):
    width = l_cores.shape[-1]
    rank_step = width // 3
    pivots, links = (
        lax.all_gather(pivot_inv, "row", axis=1, tiled=True),
        lax.all_gather(coupling, "row", axis=1, tiled=True),
    )
    positions = jnp.arange(width, dtype=jnp.int32)
    col_keep = (
        (positions[None, None, :] < (l_bucket * rank_step)[:, :, None]) & (present[:, :, None] > 0)
    ).astype(F32)
    l_masked = l_cores * col_keep[:, :, None, :]
    portion = lax.all_gather(u_cores, "row", axis=2, tiled=True)
    row_mask = (positions[None, None, :] < (u_bucket * rank_step)[:, :, None]).astype(F32)
    u_masked = portion * row_mask[..., None]
    partial_update = jnp.einsum("ikar,kjrb->ijab", l_masked, u_masked, precision=HIGH)
    own_rows = lax.psum_scatter(partial_update, "depth", scatter_dimension=2, tiled=True)
    reduced = diag_cores - own_rows
    previous = jnp.einsum("iab,bc->iac", reduced[:, 0], pivots[0], precision=HIGH)
    results = [previous]
    for column in range(1, reduced.shape[1]):
        linked = jnp.einsum("iab,bc->iac", previous, links[column - 1], precision=HIGH)
        previous = jnp.einsum(
            "iab,bc->iac", reduced[:, column] - linked, pivots[column], precision=HIGH
        )
        results.append(previous)
    return jnp.stack(results, axis=1)


def halves(value):
    high = value.astype(BF16)
    return high, (value - high.astype(F32)).astype(BF16)


def dot3(left, right_high, right_low):
    high, low = left
    dot = functools.partial(jnp.dot, preferred_element_type=F32)
    return dot(high, right_high) + (dot(high, right_low) + dot(low, right_high))


def split_lower(l_cores, l_bucket, present):
    tiles, pivots, width, _ = l_cores.shape
    step = width // 3

    def body(bucket, flags, source, high, low):
        i = pl.program_id(1)
        lane = lax.broadcasted_iota(jnp.int32, (width, width), 1)
        for side in range(2):
            k = 2 * pl.program_id(0) + side
            limit = jnp.where(flags[i, k] > 0, bucket[i, k] * step, 0)
            a, b = halves(jnp.where(lane < limit, source[0, side], 0.0))
            high[0, :, side * width : (side + 1) * width] = a
            low[0, :, side * width : (side + 1) * width] = b

    out = jax.ShapeDtypeStruct((pivots // 2, tiles * width, 2 * width), BF16)
    block = pl.BlockSpec((1, width, 2 * width), lambda p, i, *_: (p, i, 0))
    return pl.pallas_call(
        body,
        grid_spec=pltpu.PrefetchScalarGridSpec(
            num_scalar_prefetch=2,
            grid=(pivots // 2, tiles),
            in_specs=[pl.BlockSpec((1, 2, width, width), lambda p, i, *_: (i, p, 0, 0))],
            out_specs=[block, block],
        ),
        out_shape=[out, out],
        name="split_lower",
    )(l_bucket, present, l_cores)


def pack(own, twin, place):
    pivots, columns, rows, width = own.shape
    half = pivots // 2

    def body(at, mine, other, *outs):
        core = at[0] % 2
        for column in range(columns):
            outs[column][core] = mine[:, column]
            outs[column][1 - core] = other[:, column]

    source = pl.BlockSpec((1, columns, rows, width), lambda k, at: (half * (at[0] % 2) + k, 0, 0, 0))
    return pl.pallas_call(
        body,
        grid_spec=pltpu.PrefetchScalarGridSpec(
            num_scalar_prefetch=1,
            grid=(half,),
            in_specs=[source, source],
            out_specs=[pl.BlockSpec((2, 1, rows, width), lambda k, at: (0, k, 0, 0))] * columns,
        ),
        out_shape=[jax.ShapeDtypeStruct((2, half, rows, width), F32)] * columns,
        name="pack",
    )(place, own, twin)


def sources(at, bundle):
    home = at[0] - at[0] % 2
    first = jnp.where(bundle == 0, home ^ 2, home ^ 4)
    second = jnp.where(bundle == 0, home ^ 4, home ^ 2)
    return first, second, home ^ 6


def gather_tile(at, bundle, own, twin, parts, store):
    store(at[0], own)
    store(at[0] ^ 1, twin)
    for chip, part in zip(sources(at, bundle), parts):
        for core in range(2):
            store(chip + core, part(core))


def multiply(j, place, u_bucket, lower, own, twin, mine, theirs):
    high, low = lower
    pairs, height, depth = high.shape
    rows, width = own.shape[-2:]
    tiles = height // width
    step = width // 3
    half = pairs // 2
    share = width // 4

    def body(at, bucket, lhs_high, lhs_low, own_ref, twin_ref, *rest):
        parts, others = rest[:3], rest[3:6]
        keep, send, rhs_high, rhs_low, total = rest[6:]
        p = pl.program_id(0)
        core = at[0] % 2
        row = lax.broadcasted_iota(jnp.int32, (rows, width), 0)

        def assemble(refs, bundle):
            for k in range(2):
                limit = bucket[2 * p + k, j] * step

                def store(device, value):
                    start = pl.multiple_of(device * rows, 16)
                    value = jnp.where(row < limit - start, value, 0.0)
                    a, b = halves(value)
                    rhs_high[pl.ds(k * width + start, rows)] = a
                    rhs_low[pl.ds(k * width + start, rows)] = b

                gather_tile(
                    at, bundle, own_ref[k, 0], twin_ref[k, 0],
                    [lambda s, r=r: r[s, k] for r in refs], store,
                )

        @pl.when(p // half == core)
        def _():
            assemble(parts, core)

        @pl.when(p // half != core)
        def _():
            assemble(others, 1 - core)

        left = lhs_high[0], lhs_low[0]
        product = jnp.dot(
            jnp.concatenate([left[0], left[1], left[0]], axis=1),
            jnp.concatenate([rhs_high[...], rhs_high[...], rhs_low[...]], axis=0),
            preferred_element_type=F32,
        )

        @pl.when(p == 0)
        def _():
            total[...] = product

        @pl.when(p > 0)
        def _():
            total[...] += product

        @pl.when(p == pairs - 1)
        def _():
            z = at[1]
            for slot, (target, block) in enumerate(((keep, z), (keep, z ^ 2), (send, z ^ 1), (send, z ^ 3))):
                for i in range(tiles):
                    start = pl.multiple_of(block * share, 8)
                    target[slot % 2, i] = total[pl.ds(i * width + start, share)]

    lhs = pl.BlockSpec((1, height, depth), lambda p, *_: (p, 0, 0))
    local = pl.BlockSpec((2, 1, rows, width), lambda p, *_: (p, j, 0, 0))
    piece = pl.BlockSpec((2, 2, rows, width), lambda p, *_: (0, p % half, 0, 0))
    out = pl.BlockSpec((2, tiles, share, width), lambda p, *_: (0, 0, 0, 0))
    shape = jax.ShapeDtypeStruct((2, tiles, share, width), F32)
    return pl.pallas_call(
        body,
        grid_spec=pltpu.PrefetchScalarGridSpec(
            num_scalar_prefetch=2,
            grid=(pairs,),
            in_specs=[lhs, lhs, local, local] + [piece] * 6,
            out_specs=[out, out],
            scratch_shapes=[
                pltpu.VMEM((depth, width), BF16),
                pltpu.VMEM((depth, width), BF16),
                pltpu.VMEM((height, width), F32),
            ],
        ),
        out_shape=[shape, shape],
    )(place, u_bucket, high, low, own, twin, *mine, *theirs)


def finish_early(place, columns, diag, sums, own, twin, mine, theirs):
    tiles, _, share, width = diag.shape
    rows = own.shape[-2]
    half = own.shape[0] // 2
    height = tiles * share

    def body(at, *refs):
        diag_ref = refs[0]
        parts = refs[1 : 1 + 3 * (columns - 1)]
        refs = refs[1 + 3 * (columns - 1) :]
        own_ref, twin_ref, refs = refs[0], refs[1], refs[2:]
        pieces, others, refs = refs[:3], refs[3:6], refs[6:]
        done, linked_ref, last_high, last_low, mat_high, mat_low = refs
        core = at[0] % 2

        def assemble(half_index, refs, bundle):
            for local in range(half):
                k = half_index * half + local
                if k >= 2 * columns - 1:
                    continue

                def store(device, value):
                    start = pl.multiple_of(device * rows, 16)
                    a, b = halves(value)
                    mat_high[k, pl.ds(start, rows)] = a
                    mat_low[k, pl.ds(start, rows)] = b

                gather_tile(
                    at, bundle, own_ref[k, 0], twin_ref[k, 0],
                    [lambda s, r=r: r[s, local] for r in refs], store,
                )

        for half_index in range(2):
            @pl.when(core == half_index)
            def _():
                assemble(half_index, pieces, core)
                assemble(1 - half_index, others, 1 - core)

        linked = None
        for column in range(columns - 1):
            keep, near, far = (parts[3 * column + n] for n in range(3))
            reduced = (diag_ref[:, column] - (keep[0] + near[0] + far[...])).reshape(height, width)
            if linked is not None:
                reduced = reduced - linked
            previous = dot3(halves(reduced), mat_high[column], mat_low[column])
            done[:, column] = previous.reshape(tiles, share, width)
            linked = dot3(halves(previous), mat_high[columns + column], mat_low[columns + column])
        linked_ref[...] = linked.reshape(tiles, share, width)
        last_high[...] = mat_high[columns - 1]
        last_low[...] = mat_low[columns - 1]

    operands = [diag]
    for keep, near, far in sums:
        operands += [keep, near, far]
    operands += [own, twin, *mine, *theirs]
    square = jax.ShapeDtypeStruct((width, width), BF16)
    vmem = pl.BlockSpec(memory_space=pltpu.VMEM)
    return pl.pallas_call(
        body,
        in_specs=[pl.BlockSpec(memory_space=pltpu.SMEM)] + [vmem] * len(operands),
        out_specs=[vmem] * 4,
        out_shape=[
            jax.ShapeDtypeStruct((tiles, columns - 1, share, width), F32),
            jax.ShapeDtypeStruct((tiles, share, width), F32),
            square,
            square,
        ],
        scratch_shapes=[pltpu.VMEM((2 * columns - 1, width, width), BF16)] * 2,
        name="finish_early",
    )(place, *operands)


def finish_last(columns, diag, done, linked, last_high, last_low, keep, near, far):
    tiles, _, share, width = diag.shape
    height = tiles * share

    def body(diag_ref, done_ref, linked_ref, high, low, keep_ref, near_ref, far_ref, out):
        for column in range(columns - 1):
            out[:, column] = done_ref[:, column]
        reduced = diag_ref[:, columns - 1] - (keep_ref[0] + near_ref[0] + far_ref[...]) - linked_ref[...]
        value = dot3(halves(reduced.reshape(height, width)), high[...], low[...])
        out[:, columns - 1] = value.reshape(tiles, share, width)

    return pl.pallas_call(
        body,
        in_specs=[pl.BlockSpec(memory_space=pltpu.VMEM)] * 8,
        out_specs=pl.BlockSpec(memory_space=pltpu.VMEM),
        out_shape=jax.ShapeDtypeStruct(diag.shape, F32),
        name="finish_last",
    )(diag, done, linked, last_high, last_low, keep, near, far)


def moves(size, first_of_core):
    return [(d, d ^ first_of_core[d % 2]) for d in range(size)]


def cube_device(l_cores, l_bucket, present, u_cores, u_bucket, diag_cores, pivot_inv, coupling):
    columns = u_cores.shape[1]
    size = lax.axis_size("row")
    first = functools.partial(lax.ppermute, axis_name="row", perm=moves(size, (2, 4)))
    second = functools.partial(lax.ppermute, axis_name="row", perm=moves(size, (4, 2)))
    twin_of = functools.partial(lax.ppermute, axis_name="row", perm=moves(size, (1, 1)))
    deep = lax.axis_size("depth")
    near_of = functools.partial(lax.ppermute, axis_name="depth", perm=[(z, z ^ 1) for z in range(deep)])
    far_of = functools.partial(lax.ppermute, axis_name="depth", perm=[(z, z ^ 2) for z in range(deep)])
    place = jnp.stack([lax.axis_index("row"), lax.axis_index("depth")]).astype(jnp.int32)

    u_twin = twin_of(u_cores)
    small = jnp.concatenate([pivot_inv, coupling, pivot_inv[:1]], axis=0)[:, None]
    small_twin = twin_of(small)
    bundles = pack(u_cores, u_twin, place)
    lower = split_lower(l_cores, l_bucket, present)
    bundles += pack(small, small_twin, place)

    gathered = []
    for bundle in bundles:
        a = first(bundle)
        b = second(bundle)
        c = second(a)
        twins = tuple(twin_of(v) for v in (a, b, c))
        gathered.append(((a, b, c), twins))

    sums = []
    for j in range(columns):
        keep, send = multiply(j, place, u_bucket, lower, u_cores, u_twin, *gathered[j])
        near = near_of(send)
        far = far_of(keep[1] + near[1])
        sums.append((keep, near, far))
    done, linked, last_high, last_low = finish_early(
        place, columns, diag_cores, sums[:-1], small, small_twin, *gathered[columns],
    )
    return finish_last(columns, diag_cores, done, linked, last_high, last_low, *sums[-1])


def solution(mesh):
    in_specs = (
        P("row", "depth", None, None),
        P("row", "depth"),
        P("row", "depth"),
        P("depth", None, "row", None),
        P("depth", None),
        P("row", None, "depth", None),
        P(None, "row", None),
        P(None, "row", None),
    )
    out_specs = P("row", None, "depth", None)

    cube = mesh.shape["row"] == 8 and mesh.shape["depth"] == 4
    return jax.shard_map(
        cube_device if cube else plain_device,
        mesh=mesh, in_specs=in_specs, out_specs=out_specs, check_vma=False,
    )
```

```python
import functools

import jax
import jax.numpy as jnp
from jax import lax
from jax.experimental import pallas as pl
from jax.experimental.pallas import tpu as pltpu
from jax.sharding import PartitionSpec as P


HIGH = lax.Precision.HIGHEST
F32 = jnp.float32
BF16 = jnp.bfloat16
LIMIT = 16 * 2**20


def plain_device(l_cores, l_bucket, present, u_cores, u_bucket, diag_cores, pivot_inv, coupling):
    width = l_cores.shape[-1]
    rank_step = width // 3
    pivots, links = (
        lax.all_gather(pivot_inv, "row", axis=1, tiled=True),
        lax.all_gather(coupling, "row", axis=1, tiled=True),
    )
    positions = jnp.arange(width, dtype=jnp.int32)
    col_keep = (
        (positions[None, None, :] < (l_bucket * rank_step)[:, :, None]) & (present[:, :, None] > 0)
    ).astype(F32)
    l_masked = l_cores * col_keep[:, :, None, :]
    portion = lax.all_gather(u_cores, "row", axis=2, tiled=True)
    row_mask = (positions[None, None, :] < (u_bucket * rank_step)[:, :, None]).astype(F32)
    u_masked = portion * row_mask[..., None]
    partial_update = jnp.einsum("ikar,kjrb->ijab", l_masked, u_masked, precision=HIGH)
    own_rows = lax.psum_scatter(partial_update, "depth", scatter_dimension=2, tiled=True)
    reduced = diag_cores - own_rows
    previous = jnp.einsum("iab,bc->iac", reduced[:, 0], pivots[0], precision=HIGH)
    results = [previous]
    for column in range(1, reduced.shape[1]):
        linked = jnp.einsum("iab,bc->iac", previous, links[column - 1], precision=HIGH)
        previous = jnp.einsum(
            "iab,bc->iac", reduced[:, column] - linked, pivots[column], precision=HIGH
        )
        results.append(previous)
    return jnp.stack(results, axis=1)


def halves(value):
    high = value.astype(BF16)
    return high, (value - high.astype(F32)).astype(BF16)


def dot3(left, right_high, right_low):
    high, low = left
    dot = functools.partial(jnp.dot, preferred_element_type=F32)
    return dot(high, right_high) + (dot(high, right_low) + dot(low, right_high))


def split_lower(l_cores, l_bucket, present):
    tiles, pivots, width, _ = l_cores.shape
    step = width // 3

    def body(bucket, flags, source, high, low):
        i = pl.program_id(1)
        lane = lax.broadcasted_iota(jnp.int32, (width, width), 1)
        for side in range(2):
            k = 2 * pl.program_id(0) + side
            limit = jnp.where(flags[i, k] > 0, bucket[i, k] * step, 0)
            a, b = halves(jnp.where(lane < limit, source[0, side], 0.0))
            high[0, :, side * width : (side + 1) * width] = a
            low[0, :, side * width : (side + 1) * width] = b

    out = jax.ShapeDtypeStruct((pivots // 2, tiles * width, 2 * width), BF16)
    block = pl.BlockSpec((1, width, 2 * width), lambda p, i, *_: (p, i, 0))
    return pl.pallas_call(
        body,
        grid_spec=pltpu.PrefetchScalarGridSpec(
            num_scalar_prefetch=2,
            grid=(pivots // 2, tiles),
            in_specs=[pl.BlockSpec((1, 2, width, width), lambda p, i, *_: (i, p, 0, 0))],
            out_specs=[block, block],
        ),
        out_shape=[out, out],
        compiler_params=pltpu.CompilerParams(vmem_limit_bytes=LIMIT),
        name="split_lower",
    )(l_bucket, present, l_cores)


def pack(own, twin, place):
    pivots, columns, rows, width = own.shape
    half = pivots // 2

    def body(at, mine, other, *outs):
        core = at[0] % 2
        for column in range(columns):
            outs[column][core] = mine[:, column]
            outs[column][1 - core] = other[:, column]

    source = pl.BlockSpec((1, columns, rows, width), lambda k, at: (half * (at[0] % 2) + k, 0, 0, 0))
    return pl.pallas_call(
        body,
        grid_spec=pltpu.PrefetchScalarGridSpec(
            num_scalar_prefetch=1,
            grid=(half,),
            in_specs=[source, source],
            out_specs=[pl.BlockSpec((2, 1, rows, width), lambda k, at: (0, k, 0, 0))] * columns,
        ),
        out_shape=[jax.ShapeDtypeStruct((2, half, rows, width), F32)] * columns,
        compiler_params=pltpu.CompilerParams(vmem_limit_bytes=LIMIT),
        name="pack",
    )(place, own, twin)


def sources(at, bundle):
    home = at[0] - at[0] % 2
    first = jnp.where(bundle == 0, home ^ 2, home ^ 4)
    second = jnp.where(bundle == 0, home ^ 4, home ^ 2)
    return first, second, home ^ 6


def gather_tile(at, bundle, own, twin, parts, store):
    store(at[0], own)
    store(at[0] ^ 1, twin)
    for chip, part in zip(sources(at, bundle), parts):
        for core in range(2):
            store(chip + core, part(core))


def multiply(j, pieces, place, u_bucket, lower, own, twin, mine, theirs):
    high, low = lower
    pairs, height, depth = high.shape
    rows, width = own.shape[-2:]
    tiles = height // width
    step = width // 3
    half = pairs // 2
    share = width // 4
    each = tiles // pieces

    def body(at, bucket, lhs_high, lhs_low, own_ref, twin_ref, *rest):
        parts, others = rest[:3], rest[3:6]
        keep, send = rest[6 : 6 + pieces], rest[6 + pieces : 6 + 2 * pieces]
        rhs_high, rhs_low, total = rest[6 + 2 * pieces :]
        core, z = at[0] % 2, at[1]
        row = lax.broadcasted_iota(jnp.int32, (rows, width), 0)
        for turn, (bundle, refs) in enumerate(((core, parts), (1 - core, others))):
            for local in range(half):
                slot = turn * half + local
                p = bundle * half + local
                for k in range(2):
                    limit = bucket[j, 2 * p + k] * step

                    def store(device, value):
                        start = pl.multiple_of(device * rows, 16)
                        a, b = halves(jnp.where(row < limit - start, value, 0.0))
                        rhs_high[slot, pl.ds(k * width + start, rows)] = a
                        rhs_low[slot, pl.ds(k * width + start, rows)] = b

                    gather_tile(
                        at, bundle, own_ref[2 * p + k, j], twin_ref[2 * p + k, j],
                        [lambda s, r=r: r[s, 2 * local + k] for r in refs], store,
                    )
                a, b = lhs_high[p], lhs_low[p]
                product = jnp.dot(
                    jnp.concatenate([a, b, a], axis=1),
                    jnp.concatenate([rhs_high[slot], rhs_high[slot], rhs_low[slot]], axis=0),
                    preferred_element_type=F32,
                )
                if slot == 0:
                    total[...] = product
                else:
                    total[...] += product
        for slot, (target, block) in enumerate(((keep, z), (keep, z ^ 2), (send, z ^ 1), (send, z ^ 3))):
            for i in range(tiles):
                start = pl.multiple_of(block * share, 8)
                target[i // each][slot % 2, i % each] = total[pl.ds(i * width + start, share)]

    shape = jax.ShapeDtypeStruct((2, each, share, width), F32)
    vmem = pl.BlockSpec(memory_space=pltpu.VMEM)
    smem = pl.BlockSpec(memory_space=pltpu.SMEM)
    return pl.pallas_call(
        body,
        in_specs=[smem, smem] + [vmem] * 10,
        out_specs=[vmem] * (2 * pieces),
        scratch_shapes=[
            pltpu.VMEM((pairs, depth, width), BF16),
            pltpu.VMEM((pairs, depth, width), BF16),
            pltpu.VMEM((height, width), F32),
        ],
        out_shape=[shape] * (2 * pieces),
        compiler_params=pltpu.CompilerParams(vmem_limit_bytes=LIMIT),
    )(place, u_bucket, high, low, own, twin, *mine, *theirs)


def finish_early(place, columns, diag, sums, own, twin, mine, theirs):
    tiles, _, share, width = diag.shape
    rows = own.shape[-2]
    half = own.shape[0] // 2
    height = tiles * share

    def body(at, *refs):
        diag_ref = refs[0]
        parts = refs[1 : 1 + 3 * (columns - 1)]
        refs = refs[1 + 3 * (columns - 1) :]
        own_ref, twin_ref, refs = refs[0], refs[1], refs[2:]
        pieces, others, refs = refs[:3], refs[3:6], refs[6:]
        done, linked_ref, last_high, last_low, mat_high, mat_low = refs
        core = at[0] % 2

        def assemble(half_index, refs, bundle):
            for local in range(half):
                k = half_index * half + local
                if k >= 2 * columns - 1:
                    continue

                def store(device, value):
                    start = pl.multiple_of(device * rows, 16)
                    a, b = halves(value)
                    mat_high[k, pl.ds(start, rows)] = a
                    mat_low[k, pl.ds(start, rows)] = b

                gather_tile(
                    at, bundle, own_ref[k, 0], twin_ref[k, 0],
                    [lambda s, r=r: r[s, local] for r in refs], store,
                )

        for half_index in range(2):
            @pl.when(core == half_index)
            def _():
                assemble(half_index, pieces, core)
                assemble(1 - half_index, others, 1 - core)

        linked = None
        for column in range(columns - 1):
            keep, near, far = (parts[3 * column + n] for n in range(3))
            reduced = (diag_ref[:, column] - (keep[0] + near[0] + far[...])).reshape(height, width)
            if linked is not None:
                reduced = reduced - linked
            previous = dot3(halves(reduced), mat_high[column], mat_low[column])
            done[:, column] = previous.reshape(tiles, share, width)
            linked = dot3(halves(previous), mat_high[columns + column], mat_low[columns + column])
        linked_ref[...] = linked.reshape(tiles, share, width)
        last_high[...] = mat_high[columns - 1]
        last_low[...] = mat_low[columns - 1]

    operands = [diag]
    for keep, near, far in sums:
        operands += [keep, near, far]
    operands += [own, twin, *mine, *theirs]
    square = jax.ShapeDtypeStruct((width, width), BF16)
    vmem = pl.BlockSpec(memory_space=pltpu.VMEM)
    return pl.pallas_call(
        body,
        in_specs=[pl.BlockSpec(memory_space=pltpu.SMEM)] + [vmem] * len(operands),
        out_specs=[vmem] * 4,
        out_shape=[
            jax.ShapeDtypeStruct((tiles, columns - 1, share, width), F32),
            jax.ShapeDtypeStruct((tiles, share, width), F32),
            square,
            square,
        ],
        scratch_shapes=[pltpu.VMEM((2 * columns - 1, width, width), BF16)] * 2,
        compiler_params=pltpu.CompilerParams(vmem_limit_bytes=LIMIT),
        name="finish_early",
    )(place, *operands)


def finish_last(columns, diag, done, linked, last_high, last_low, parts):
    tiles, _, share, width = diag.shape
    each = tiles // len(parts)
    height = each * share

    def body(diag_ref, done_ref, linked_ref, high, low, *rest):
        out = rest[-1]
        for column in range(columns - 1):
            out[:, column] = done_ref[:, column]
        for n in range(len(parts)):
            keep, near, far = rest[3 * n : 3 * n + 3]
            span = slice(n * each, (n + 1) * each)
            update = keep[0] + near[0] + far[...]
            reduced = diag_ref[span, columns - 1] - update - linked_ref[span]
            value = dot3(halves(reduced.reshape(height, width)), high[...], low[...])
            out[span, columns - 1] = value.reshape(each, share, width)

    return pl.pallas_call(
        body,
        in_specs=[pl.BlockSpec(memory_space=pltpu.VMEM)] * (5 + 3 * len(parts)),
        out_specs=pl.BlockSpec(memory_space=pltpu.VMEM),
        out_shape=jax.ShapeDtypeStruct(diag.shape, F32),
        compiler_params=pltpu.CompilerParams(vmem_limit_bytes=LIMIT),
        name="finish_last",
    )(diag, done, linked, last_high, last_low, *[v for part in parts for v in part])


def moves(size, first_of_core):
    return [(d, d ^ first_of_core[d % 2]) for d in range(size)]


def cube_device(l_cores, l_bucket, present, u_cores, u_bucket, diag_cores, pivot_inv, coupling):
    columns, tiles = u_cores.shape[1], l_cores.shape[0]
    size = lax.axis_size("row")
    first = functools.partial(lax.ppermute, axis_name="row", perm=moves(size, (2, 4)))
    second = functools.partial(lax.ppermute, axis_name="row", perm=moves(size, (4, 2)))
    twin_of = functools.partial(lax.ppermute, axis_name="row", perm=moves(size, (1, 1)))
    deep = lax.axis_size("depth")
    near_of = functools.partial(lax.ppermute, axis_name="depth", perm=[(z, z ^ 1) for z in range(deep)])
    far_of = functools.partial(lax.ppermute, axis_name="depth", perm=[(z, z ^ 2) for z in range(deep)])
    place = jnp.stack([lax.axis_index("row"), lax.axis_index("depth")]).astype(jnp.int32)

    u_twin = twin_of(u_cores)
    small = jnp.concatenate([pivot_inv, coupling, pivot_inv[:1]], axis=0)[:, None]
    small_twin = twin_of(small)
    bundles = pack(u_cores, u_twin, place)
    lower = split_lower(l_cores, l_bucket, present)
    bundles += pack(small, small_twin, place)

    gathered = []
    for bundle in bundles:
        a = first(bundle)
        b = second(bundle)
        c = second(a)
        twins = tuple(twin_of(v) for v in (a, b, c))
        gathered.append(((a, b, c), twins))

    sums = []
    bucket = u_bucket.T
    for j in range(columns):
        pieces = tiles if j == columns - 1 else 1
        outs = multiply(j, pieces, place, bucket, lower, u_cores, u_twin, *gathered[j])
        parts = []
        for n in range(pieces):
            keep, send = outs[n], outs[pieces + n]
            near = near_of(send)
            far = far_of(keep[1] + near[1])
            parts.append((keep, near, far))
        sums.append(parts)
    done, linked, last_high, last_low = finish_early(
        place, columns, diag_cores, [p[0] for p in sums[:-1]], small, small_twin, *gathered[columns],
    )
    return finish_last(columns, diag_cores, done, linked, last_high, last_low, sums[-1])


def solution(mesh):
    in_specs = (
        P("row", "depth", None, None),
        P("row", "depth"),
        P("row", "depth"),
        P("depth", None, "row", None),
        P("depth", None),
        P("row", None, "depth", None),
        P(None, "row", None),
        P(None, "row", None),
    )
    out_specs = P("row", None, "depth", None)

    cube = mesh.shape["row"] == 8 and mesh.shape["depth"] == 4
    return jax.shard_map(
        cube_device if cube else plain_device,
        mesh=mesh, in_specs=in_specs, out_specs=out_specs, check_vma=False,
    )
```

```python
import functools

import jax
import jax.numpy as jnp
from jax import lax
from jax.experimental import pallas as pl
from jax.experimental.pallas import tpu as pltpu
from jax.sharding import PartitionSpec as P


HIGH = lax.Precision.HIGHEST
F32 = jnp.float32
BF16 = jnp.bfloat16
LIMIT = 16 * 2**20


def plain_device(l_cores, l_bucket, present, u_cores, u_bucket, diag_cores, pivot_inv, coupling):
    width = l_cores.shape[-1]
    rank_step = width // 3
    pivots, links = (
        lax.all_gather(pivot_inv, "row", axis=1, tiled=True),
        lax.all_gather(coupling, "row", axis=1, tiled=True),
    )
    positions = jnp.arange(width, dtype=jnp.int32)
    col_keep = (
        (positions[None, None, :] < (l_bucket * rank_step)[:, :, None]) & (present[:, :, None] > 0)
    ).astype(F32)
    l_masked = l_cores * col_keep[:, :, None, :]
    portion = lax.all_gather(u_cores, "row", axis=2, tiled=True)
    row_mask = (positions[None, None, :] < (u_bucket * rank_step)[:, :, None]).astype(F32)
    u_masked = portion * row_mask[..., None]
    partial_update = jnp.einsum("ikar,kjrb->ijab", l_masked, u_masked, precision=HIGH)
    own_rows = lax.psum_scatter(partial_update, "depth", scatter_dimension=2, tiled=True)
    reduced = diag_cores - own_rows
    previous = jnp.einsum("iab,bc->iac", reduced[:, 0], pivots[0], precision=HIGH)
    results = [previous]
    for column in range(1, reduced.shape[1]):
        linked = jnp.einsum("iab,bc->iac", previous, links[column - 1], precision=HIGH)
        previous = jnp.einsum(
            "iab,bc->iac", reduced[:, column] - linked, pivots[column], precision=HIGH
        )
        results.append(previous)
    return jnp.stack(results, axis=1)


def halves(value):
    high = value.astype(BF16)
    return high, (value - high.astype(F32)).astype(BF16)


def dot3(left, right_high, right_low):
    high, low = left
    dot = functools.partial(jnp.dot, preferred_element_type=F32)
    return dot(high, right_high) + (dot(high, right_low) + dot(low, right_high))


def split_lower(l_cores, l_bucket, present):
    tiles, pivots, width, _ = l_cores.shape
    step = width // 3

    def body(bucket, flags, source, high, low):
        i = pl.program_id(1)
        lane = lax.broadcasted_iota(jnp.int32, (width, width), 1)
        for side in range(2):
            k = 2 * pl.program_id(0) + side
            limit = jnp.where(flags[i, k] > 0, bucket[i, k] * step, 0)
            a, b = halves(jnp.where(lane < limit, source[0, side], 0.0))
            high[0, :, side * width : (side + 1) * width] = a
            low[0, :, side * width : (side + 1) * width] = b

    out = jax.ShapeDtypeStruct((pivots // 2, tiles * width, 2 * width), BF16)
    block = pl.BlockSpec((1, width, 2 * width), lambda p, i, *_: (p, i, 0))
    return pl.pallas_call(
        body,
        grid_spec=pltpu.PrefetchScalarGridSpec(
            num_scalar_prefetch=2,
            grid=(pivots // 2, tiles),
            in_specs=[pl.BlockSpec((1, 2, width, width), lambda p, i, *_: (i, p, 0, 0))],
            out_specs=[block, block],
        ),
        out_shape=[out, out],
        compiler_params=pltpu.CompilerParams(vmem_limit_bytes=LIMIT),
        name="split_lower",
    )(l_bucket, present, l_cores)


def pack(own, twin, place, chunks):
    half, rows = own.shape[0] // 2, own.shape[2]

    def body(at, mine, other, *outs):
        core = at[0] % 2
        for (column, lane, lanes), out in zip(chunks, outs):
            for k in range(half):
                out[core, k] = mine[half * core + k, column, :, lane : lane + lanes]
                out[1 - core, k] = other[half * core + k, column, :, lane : lane + lanes]

    vmem = pl.BlockSpec(memory_space=pltpu.VMEM)
    return pl.pallas_call(
        body,
        in_specs=[pl.BlockSpec(memory_space=pltpu.SMEM), vmem, vmem],
        out_specs=[vmem] * len(chunks),
        out_shape=[jax.ShapeDtypeStruct((2, half, rows, lanes), F32) for _, _, lanes in chunks],
        compiler_params=pltpu.CompilerParams(vmem_limit_bytes=LIMIT),
        name="pack",
    )(place, own, twin)


def sources(at, bundle):
    home = at[0] - at[0] % 2
    first = jnp.where(bundle == 0, home ^ 2, home ^ 4)
    second = jnp.where(bundle == 0, home ^ 4, home ^ 2)
    return first, second, home ^ 6


def gather_tile(at, bundle, own, twin, parts, store):
    store(at[0], own)
    store(at[0] ^ 1, twin)
    for chip, part in zip(sources(at, bundle), parts):
        for core in range(2):
            store(chip + core, part(core))


def multiply(chunk, place, u_bucket, lower, own, twin, mine, theirs):
    j, lane, lanes = chunk
    high, low = lower
    pairs, height, depth = high.shape
    rows, width = own.shape[-2:]
    tiles = height // width
    step = width // 3
    half = pairs // 2
    share = width // 4

    def body(at, bucket, lhs_high, lhs_low, own_ref, twin_ref, *rest):
        parts, others = rest[:3], rest[3:6]
        keep, send, (rhs_high, rhs_low, total) = rest[6:8], rest[8:10], rest[10:]
        core, z = at[0] % 2, at[1]
        row = lax.broadcasted_iota(jnp.int32, (rows, lanes), 0)
        span = slice(lane, lane + lanes)
        for turn, (bundle, refs) in enumerate(((core, parts), (1 - core, others))):
            for local in range(half):
                slot = turn * half + local
                p = bundle * half + local
                for k in range(2):
                    limit = bucket[j, 2 * p + k] * step

                    def store(device, value):
                        start = pl.multiple_of(device * rows, 16)
                        a, b = halves(jnp.where(row < limit - start, value, 0.0))
                        rhs_high[slot, pl.ds(k * width + start, rows)] = a
                        rhs_low[slot, pl.ds(k * width + start, rows)] = b

                    gather_tile(
                        at, bundle, own_ref[2 * p + k, j, :, span], twin_ref[2 * p + k, j, :, span],
                        [lambda s, r=r: r[s, 2 * local + k] for r in refs], store,
                    )
                a, b = lhs_high[p], lhs_low[p]
                product = jnp.dot(
                    jnp.concatenate([a, b, a], axis=1),
                    jnp.concatenate([rhs_high[slot], rhs_high[slot], rhs_low[slot]], axis=0),
                    preferred_element_type=F32,
                )
                if slot == 0:
                    total[...] = product
                else:
                    total[...] += product
        for slot, (target, block) in enumerate(((keep, z), (keep, z ^ 2), (send, z ^ 1), (send, z ^ 3))):
            for i in range(tiles):
                start = pl.multiple_of(block * share, 8)
                target[slot % 2][i] = total[pl.ds(i * width + start, share)]

    shape = jax.ShapeDtypeStruct((tiles, share, lanes), F32)
    vmem = pl.BlockSpec(memory_space=pltpu.VMEM)
    smem = pl.BlockSpec(memory_space=pltpu.SMEM)
    return pl.pallas_call(
        body,
        in_specs=[smem, smem] + [vmem] * 10,
        out_specs=[vmem] * 4,
        scratch_shapes=[
            pltpu.VMEM((pairs, depth, lanes), BF16),
            pltpu.VMEM((pairs, depth, lanes), BF16),
            pltpu.VMEM((height, lanes), F32),
        ],
        out_shape=[shape] * 4,
        compiler_params=pltpu.CompilerParams(vmem_limit_bytes=LIMIT),
    )(place, u_bucket, high, low, own, twin, *mine, *theirs)


def joined(parts):
    terms = [parts[n][...] + parts[n + 1][...] + parts[n + 2][...] for n in range(0, len(parts), 3)]
    return terms[0] if len(terms) == 1 else jnp.concatenate(terms, axis=-1)


def finish_early(place, columns, diag, sums, own, twin, mine, theirs):
    tiles, _, share, width = diag.shape
    rows = own.shape[-2]
    half = own.shape[0] // 2
    height = tiles * share
    count = sum(len(part) for part in sums)

    def body(at, *refs):
        diag_ref = refs[0]
        parts, refs = refs[1 : 1 + 3 * count], refs[1 + 3 * count :]
        own_ref, twin_ref, refs = refs[0], refs[1], refs[2:]
        pieces, others, refs = refs[:3], refs[3:6], refs[6:]
        done, linked_ref, last_high, last_low, mat_high, mat_low = refs
        core = at[0] % 2

        def assemble(half_index, refs, bundle):
            for local in range(half):
                k = half_index * half + local
                if k >= 2 * columns - 1:
                    continue

                def store(device, value):
                    start = pl.multiple_of(device * rows, 16)
                    a, b = halves(value)
                    mat_high[k, pl.ds(start, rows)] = a
                    mat_low[k, pl.ds(start, rows)] = b

                gather_tile(
                    at, bundle, own_ref[k, 0], twin_ref[k, 0],
                    [lambda s, r=r: r[s, local] for r in refs], store,
                )

        for half_index in range(2):
            @pl.when(core == half_index)
            def _():
                assemble(half_index, pieces, core)
                assemble(1 - half_index, others, 1 - core)

        linked = None
        for column in range(columns - 1):
            first = 3 * sum(len(part) for part in sums[:column])
            update = joined(parts[first : first + 3 * len(sums[column])])
            reduced = (diag_ref[:, column] - update).reshape(height, width)
            if linked is not None:
                reduced = reduced - linked
            previous = dot3(halves(reduced), mat_high[column], mat_low[column])
            done[:, column] = previous.reshape(tiles, share, width)
            linked = dot3(halves(previous), mat_high[columns + column], mat_low[columns + column])
        linked_ref[...] = linked.reshape(tiles, share, width)
        last_high[...] = mat_high[columns - 1]
        last_low[...] = mat_low[columns - 1]

    operands = [diag]
    for part in sums:
        operands += [value for chunk in part for value in chunk]
    operands += [own, twin, *mine, *theirs]
    square = jax.ShapeDtypeStruct((width, width), BF16)
    vmem = pl.BlockSpec(memory_space=pltpu.VMEM)
    return pl.pallas_call(
        body,
        in_specs=[pl.BlockSpec(memory_space=pltpu.SMEM)] + [vmem] * len(operands),
        out_specs=[vmem] * 4,
        out_shape=[
            jax.ShapeDtypeStruct((tiles, columns - 1, share, width), F32),
            jax.ShapeDtypeStruct((tiles, share, width), F32),
            square,
            square,
        ],
        scratch_shapes=[pltpu.VMEM((2 * columns - 1, width, width), BF16)] * 2,
        compiler_params=pltpu.CompilerParams(vmem_limit_bytes=LIMIT),
        name="finish_early",
    )(place, *operands)


def finish_last(columns, diag, done, linked, last_high, last_low, parts):
    tiles, _, share, width = diag.shape
    height = tiles * share

    def body(diag_ref, done_ref, linked_ref, high, low, *rest):
        out = rest[-1]
        for column in range(columns - 1):
            out[:, column] = done_ref[:, column]
        reduced = diag_ref[:, columns - 1] - joined(rest[:-1]) - linked_ref[...]
        value = dot3(halves(reduced.reshape(height, width)), high[...], low[...])
        out[:, columns - 1] = value.reshape(tiles, share, width)

    return pl.pallas_call(
        body,
        in_specs=[pl.BlockSpec(memory_space=pltpu.VMEM)] * (5 + 3 * len(parts)),
        out_specs=pl.BlockSpec(memory_space=pltpu.VMEM),
        out_shape=jax.ShapeDtypeStruct(diag.shape, F32),
        compiler_params=pltpu.CompilerParams(vmem_limit_bytes=LIMIT),
        name="finish_last",
    )(diag, done, linked, last_high, last_low, *[v for part in parts for v in part])


def moves(size, first_of_core):
    return [(d, d ^ first_of_core[d % 2]) for d in range(size)]


def chunks_of(columns, width):
    step = width // 3
    last = columns - 1
    return [(column, 0, width) for column in range(last)] + [(last, 0, 2 * step), (last, 2 * step, step)]


def cube_device(l_cores, l_bucket, present, u_cores, u_bucket, diag_cores, pivot_inv, coupling):
    columns = u_cores.shape[1]
    size = lax.axis_size("row")
    first = functools.partial(lax.ppermute, axis_name="row", perm=moves(size, (2, 4)))
    second = functools.partial(lax.ppermute, axis_name="row", perm=moves(size, (4, 2)))
    twin_of = functools.partial(lax.ppermute, axis_name="row", perm=moves(size, (1, 1)))
    deep = lax.axis_size("depth")
    near_of = functools.partial(lax.ppermute, axis_name="depth", perm=[(z, z ^ 1) for z in range(deep)])
    far_of = functools.partial(lax.ppermute, axis_name="depth", perm=[(z, z ^ 2) for z in range(deep)])
    place = jnp.stack([lax.axis_index("row"), lax.axis_index("depth")]).astype(jnp.int32)

    u_twin = twin_of(u_cores)
    small = jnp.concatenate([pivot_inv, coupling, pivot_inv[:1]], axis=0)[:, None]
    small_twin = twin_of(small)
    width = u_cores.shape[-1]
    chunks = chunks_of(columns, width)
    bundles = pack(u_cores, u_twin, place, chunks)
    lower = split_lower(l_cores, l_bucket, present)
    bundles += pack(small, small_twin, place, [(0, 0, width)])

    gathered = []
    for bundle in bundles:
        a = first(bundle)
        b = second(bundle)
        c = second(a)
        twins = tuple(twin_of(v) for v in (a, b, c))
        gathered.append(((a, b, c), twins))

    sums = [[] for _ in range(columns)]
    bucket = u_bucket.T
    for n, chunk in enumerate(chunks):
        own, relayed, send, onward = multiply(chunk, place, bucket, lower, u_cores, u_twin, *gathered[n])
        far = far_of(relayed + near_of(onward))
        sums[chunk[0]].append((own, near_of(send), far))
    done, linked, last_high, last_low = finish_early(
        place, columns, diag_cores, sums[:-1], small, small_twin, *gathered[len(chunks)],
    )
    return finish_last(columns, diag_cores, done, linked, last_high, last_low, sums[-1])


def solution(mesh):
    in_specs = (
        P("row", "depth", None, None),
        P("row", "depth"),
        P("row", "depth"),
        P("depth", None, "row", None),
        P("depth", None),
        P("row", None, "depth", None),
        P(None, "row", None),
        P(None, "row", None),
    )
    out_specs = P("row", None, "depth", None)

    cube = mesh.shape["row"] == 8 and mesh.shape["depth"] == 4
    return jax.shard_map(
        cube_device if cube else plain_device,
        mesh=mesh, in_specs=in_specs, out_specs=out_specs, check_vma=False,
    )
```
